128 devices in a mesh: ctx: 16 (over z_lo, y, core), head: 8 (over x, z_hi).
Axes of the slice: x: 4, y: 4, z: 4 (z_hi: 2, z_lo: 2; z = z_hi * 2 + z_lo), core: 2. Of those that a mesh axis runs over, the one named last changes fastest.
Arguments:
- queries: bfloat16 [16384, 6144], P(('ctx', 'head')), may hold values from -56 to 56
- key_rows: bfloat16 [16384, 6144], P(('ctx', 'head')), may hold values from -6 to 6
- value_rows: bfloat16 [16384, 6144], P(('ctx', 'head')), may hold values from -6 to 6
- key_tiles: int32 [48, 128, 18], P('head', 'ctx'), may hold values from -1 to 127, as said below
Outputs:
- attended: bfloat16 [16384, 6144], P(('ctx', 'head'))
The draws below stay inside these ranges and needn't reach their ends.
Inputs may be any that keep to these rules, and one draw needn't show every extreme that they name: In key_tiles[h, i] the live slots come first and name distinct tiles whose time slab differs from tile i's by at most one; the rest hold -1. Tile i itself and the tiles of the same cell one time slab before and after (where they exist) are always live. In every draw some head and tile have all 18 slots live.
All inputs are finite; a program needn't handle non-finite values.
Results may differ from the reference program's by a relative error of at most 0.0046.
Values may be sent and summed in bfloat16 or wider, within the bound.
A program may use at most 128 MiB of HBM per device.

```python
import jax
import jax.numpy as jnp
from jax import lax

H = 48
HDIM = 128
D = 6144
TILE = 128
GY = 2
GX = 4
KT = 18
NTT = 16
NTILES = 128
TOKENS = 16384


def paired_rows(key):
    seed_base = jax.random.fold_in(key, 5)
    seed_query, seed_keys = jax.random.split(seed_base, 2)
    query_all = jnp.clip(jax.random.normal(seed_query, (TOKENS, D), jnp.float32), -6.0, 6.0)
    keys_all = jnp.clip(jax.random.normal(seed_keys, (TOKENS, D), jnp.float32), -6.0, 6.0)
    return (query_all, keys_all)


def draw_queries(key, part):
    return paired_rows(key)[0].astype(jnp.bfloat16)


def draw_key_rows(key, part):
    return paired_rows(key)[1].astype(jnp.bfloat16)


def draw_key_tiles(key, part):
    seed_base = jax.random.fold_in(key, 11)
    seed_y, seed_x, seed_wide = jax.random.split(seed_base, 3)
    reach_y = jax.random.randint(seed_y, (H,), 0, 2)
    reach_x = jax.random.randint(seed_x, (H,), 0, 2)
    wide_head = jax.random.randint(seed_wide, (), 0, H)
    reach_y = reach_y.at[wide_head].set(1)
    reach_x = reach_x.at[wide_head].set(1)
    cells = GY * GX
    tile_ids = jnp.arange(NTILES)
    slab_of = tile_ids // cells
    row_of = tile_ids % cells // GX
    col_of = tile_ids % GX
    offsets = jnp.arange(27)
    step_t = offsets // 9 - 1
    step_y = offsets // 3 % 3 - 1
    step_x = offsets % 3 - 1
    near_slab = slab_of[:, None] + step_t[None, :]
    near_row = row_of[:, None] + step_y[None, :]
    near_col = col_of[:, None] + step_x[None, :]
    inside = (near_slab >= 0) & (near_slab < NTT) & (near_row >= 0) & (near_row < GY) & (near_col >= 0) & (near_col < GX)
    within = (jnp.abs(step_y)[None, None, :] <= reach_y[:, None, None]) & (jnp.abs(step_x)[None, None, :] <= reach_x[:, None, None])
    usable = inside[None, :, :] & within
    target = near_slab * cells + near_row * GX + near_col
    ranking = jnp.where(usable, offsets[None, None, :], 27 + offsets[None, None, :])
    order_ids = jnp.argsort(ranking, axis=-1, stable=True)[..., :KT]
    chosen = jnp.take_along_axis(jnp.broadcast_to(target[None], usable.shape), order_ids, axis=-1)
    chosen_ok = jnp.take_along_axis(usable, order_ids, axis=-1)
    return jnp.where(chosen_ok, chosen, -1).astype(jnp.int32)


def level_of(own_key, dims, cuts, low, top_value):
    def one(dim, shards_of):
        steps = jax.random.uniform(jax.random.fold_in(jax.random.fold_in(own_key, 6), dim), (shards_of,), jnp.float32, low / len(cuts), top_value / len(cuts))
        return jnp.repeat(jnp.exp(steps), dims[dim] // shards_of).reshape((-1,) + (1,) * (len(dims) - dim - 1))

    level = one(*cuts[0])
    for cut in cuts[1:]:
        level = level * one(*cut)
    return level


def gaussian(own_key, dims, width, reach, pieces=(), held_as=jnp.bfloat16):
    values = jax.random.normal(own_key, dims, jnp.float32) * width
    if len(pieces) > 0:
        values = level_of(own_key, dims, pieces, -0.22, 0.18) * values
    return jnp.clip(values, min=-reach, max=reach).astype(held_as)


def setup_inputs(seed: int = 0) -> dict:
    splits = jax.random.split(jax.random.key(seed), 5)
    return {
        "queries": draw_queries(jax.random.fold_in(splits[4], 71), 0),
        "key_rows": draw_key_rows(jax.random.fold_in(splits[4], 71), 0),
        "value_rows": gaussian(splits[2], (TOKENS, D), 1.0, 6.0, ((0, 128),)),
        "key_tiles": draw_key_tiles(jax.random.fold_in(splits[4], 71), 0),
    }


def one_head(operands):
    head_query, head_keys, head_values, listed = operands
    is_live = listed >= 0
    safe_ids = jnp.where(is_live, listed, 0).astype(jnp.int32)
    picked_keys = head_keys[safe_ids].astype(jnp.float32)
    picked_values = head_values[safe_ids].astype(jnp.float32)
    scores = jnp.einsum("qtd,qksd->qtks", head_query.astype(jnp.float32), picked_keys, precision=lax.Precision.HIGHEST) * (HDIM ** -0.5)
    live_mask = is_live[:, None, :, None]
    scores = jnp.where(live_mask, scores, jnp.float32(-1e30))
    row_max = jnp.max(scores, axis=(2, 3), keepdims=True)
    weight = jnp.where(live_mask, jnp.exp(scores - row_max), jnp.float32(0.0))
    row_total = jnp.sum(weight, axis=(2, 3))
    probs = lax.optimization_barrier(weight.astype(jnp.bfloat16))
    numerator = jnp.einsum("qtks,qksd->qtd", probs.astype(jnp.float32), picked_values, precision=lax.Precision.HIGHEST)
    return (numerator / row_total[..., None]).astype(jnp.bfloat16)


def by_head(array):
    return array.reshape(NTILES, TILE, H, HDIM).transpose(2, 0, 1, 3)


def reference(queries, key_rows, value_rows, key_tiles):
    result = lax.map(one_head, (by_head(queries), by_head(key_rows), by_head(value_rows), key_tiles))
    return result.transpose(1, 2, 0, 3).reshape(TOKENS, H * HDIM)
```

```python
import functools
import math

import jax
import jax.numpy as jnp
from jax import lax
from jax.experimental import pallas as pl
from jax.experimental.pallas import tpu as pltpu
from jax.sharding import PartitionSpec as P

HDIM = 128
TILE = 128
MESH = pl.DeviceIdType.MESH
MASKED = -1e30
EXP2_SCALE = HDIM ** -0.5 / math.log(2.0)


def attend(tiles_ref, qb, work, sc, ob, j, t, base, own):
    slots = tiles_ref.shape[2]
    query = qb[j, t]
    ids, bias = [], []
    for s in range(slots):
        listed = tiles_ref[j, t, s]
        live = listed >= 0
        ids.append(jnp.clip(jnp.where(live, listed - base, own), 0, 3 * own - 1))
        bias.append(jnp.where(live, 0.0, MASKED))
    top = None
    for s in range(0, slots, 2):
        keys = jnp.concatenate([work[0, ids[s]], work[0, ids[s + 1]]], axis=0)
        scores = lax.dot_general(query, keys, (((1,), (1,)), ((), ())), preferred_element_type=jnp.float32)
        first = scores[:, :TILE] + bias[s]
        second = scores[:, TILE:] + bias[s + 1]
        sc[s] = first
        sc[s + 1] = second
        pair = jnp.maximum(first, second)
        top = pair if top is None else jnp.maximum(top, pair)
    row_max = jnp.max(top, axis=1, keepdims=True)
    total, numerator = None, None
    for s in range(0, slots, 2):
        first = jnp.exp2((sc[s] - row_max) * EXP2_SCALE)
        second = jnp.exp2((sc[s + 1] - row_max) * EXP2_SCALE)
        pair = first + second
        total = pair if total is None else total + pair
        probs = jnp.concatenate([first.astype(jnp.bfloat16), second.astype(jnp.bfloat16)], axis=1)
        values = jnp.concatenate([work[1, ids[s]], work[1, ids[s + 1]]], axis=0)
        part = jnp.dot(probs, values, preferred_element_type=jnp.float32)
        numerator = part if numerator is None else numerator + part
    row_total = jnp.sum(total, axis=1, keepdims=True)
    ob[j, t] = (numerator / row_total).astype(jnp.bfloat16)


def kernel(n_ctx, n_head, tiles_ref, q_ref, k_ref, v_ref, out_ref, qb, kvb, ob, work, sc, send_in, send_halo, send_out, recv_kv, recv_q, recv_halo, recv_out):
    heads = tiles_ref.shape[0]
    c, me = lax.axis_index("ctx"), lax.axis_index("head")
    before, after = lax.rem(c + n_ctx - 1, n_ctx), lax.rem(c + 1, n_ctx)
    base = (c - 1) * n_head

    def columns(group, j):
        return pl.ds(pl.multiple_of((group * heads + j) * HDIM, HDIM), HDIM)

    barrier = pltpu.get_barrier_semaphore()
    for p in range(1, n_head):
        pl.semaphore_signal(barrier, inc=1, device_id=(c, lax.rem(me + p, n_head)), device_id_type=MESH)
    for other in (before, after):
        pl.semaphore_signal(barrier, inc=1, device_id=(other, me), device_id_type=MESH)
    pl.semaphore_wait(barrier, n_head + 1)

    def send_tile(source, place, j, sem_index, recv):
        for p in range(1, n_head):
            peer = lax.rem(me + p, n_head)
            pltpu.make_async_remote_copy(
                src_ref=source.at[:, columns(peer, j)], dst_ref=place(), send_sem=send_in.at[sem_index],
                recv_sem=recv, device_id=(c, peer), device_id_type=MESH,
            ).start()
        pltpu.make_async_copy(source.at[:, columns(me, j)], place(), recv).start()

    def send_kv(j):
        send_tile(k_ref, lambda: kvb.at[j, 0, n_head + me], j, 0, recv_kv.at[j])
        send_tile(v_ref, lambda: kvb.at[j, 1, n_head + me], j, 1, recv_kv.at[j])

    def send_q(j):
        send_tile(q_ref, lambda: qb.at[j, me], j, 2, recv_q.at[j])

    send_kv(0)

    @pl.loop(0, heads)
    def _(j):
        @pl.when(j + 1 < heads)
        def _():
            send_kv(j + 1)

        send_q(j)

    def pass_halo(j):
        own = kvb.at[j, :, pl.ds(n_head, n_head)]
        pltpu.make_async_copy(own, own, recv_kv.at[j]).wait()
        for other, slot in ((after, 0), (before, 2 * n_head)):
            pltpu.make_async_remote_copy(
                src_ref=own, dst_ref=kvb.at[j, :, pl.ds(slot, n_head)], send_sem=send_halo,
                recv_sem=recv_halo.at[j], device_id=(other, me), device_id_type=MESH,
            ).start()

    def return_tile(j, t):
        place = out_ref.at[:, columns(me, j)]

        @pl.when(t == me)
        def _():
            pltpu.make_async_copy(ob.at[j, t], place, recv_out).start()

        @pl.when(t != me)
        def _():
            pltpu.make_async_remote_copy(
                src_ref=ob.at[j, t], dst_ref=place, send_sem=send_out,
                recv_sem=recv_out, device_id=(c, t), device_id_type=MESH,
            ).start()

    pass_halo(0)

    @pl.loop(0, heads)
    def _(j):
        @pl.when(j + 1 < heads)
        def _():
            pass_halo(j + 1)

        both = kvb.at[j, :, pl.ds(0, 2 * n_head)]
        pltpu.make_async_copy(both, both, recv_halo.at[j]).wait()
        pltpu.make_async_copy(qb.at[j], qb.at[j], recv_q.at[j]).wait()

        @pl.loop(0, 3 * n_head)
        def _(i):
            work[0, i] = kvb[j, 0, i]
            work[1, i] = kvb[j, 1, i]

        @pl.loop(0, n_head)
        def _(i):
            t = lax.rem(me + 1 + i, n_head)
            attend(tiles_ref, qb, work, sc, ob, j, t, base, n_head)

            @pl.when(i > 0)
            def _():
                return_tile(j, lax.rem(me + i, n_head))

        return_tile(j, me)

    sent = qb.at[:, pl.ds(0, n_head - 1)]
    for i in range(3):
        pltpu.make_async_copy(sent, sent, send_in.at[i]).wait()
    halo = kvb.at[:, :, pl.ds(0, 2 * n_head)]
    pltpu.make_async_copy(halo, halo, send_halo).wait()
    pltpu.make_async_copy(sent, sent, send_out).wait()
    pltpu.make_async_copy(out_ref, out_ref, recv_out).wait()


def solution(mesh):
    n_ctx, n_head = mesh.shape["ctx"], mesh.shape["head"]

    def shards(queries, key_rows, value_rows, key_tiles):
        heads, _, slots = key_tiles.shape
        return pl.pallas_call(
            functools.partial(kernel, n_ctx, n_head),
            out_shape=jax.ShapeDtypeStruct(queries.shape, queries.dtype),
            in_specs=[pl.BlockSpec(memory_space=pltpu.SMEM)] + [pl.BlockSpec(memory_space=pltpu.HBM)] * 3,
            out_specs=pl.BlockSpec(memory_space=pltpu.HBM),
            scratch_shapes=[
                pltpu.VMEM((heads, n_head, TILE, HDIM), jnp.bfloat16),
                pltpu.VMEM((heads, 2, 3 * n_head, TILE, HDIM), jnp.bfloat16),
                pltpu.VMEM((heads, n_head, TILE, HDIM), jnp.bfloat16),
                pltpu.VMEM((2, 3 * n_head, TILE, HDIM), jnp.bfloat16),
                pltpu.VMEM((slots, TILE, TILE), jnp.float32),
                pltpu.SemaphoreType.DMA((3,)),
                pltpu.SemaphoreType.DMA,
                pltpu.SemaphoreType.DMA,
                pltpu.SemaphoreType.DMA((heads,)),
                pltpu.SemaphoreType.DMA((heads,)),
                pltpu.SemaphoreType.DMA((heads,)),
                pltpu.SemaphoreType.DMA,
            ],
            compiler_params=pltpu.CompilerParams(
                collective_id=0, has_side_effects=True, vmem_limit_bytes=48 * 1024 * 1024
            ),
        )(key_tiles, queries, key_rows, value_rows)

    return jax.shard_map(
        shards,
        mesh=mesh,
        in_specs=(P(("ctx", "head"), None), P(("ctx", "head"), None), P(("ctx", "head"), None), P("head", "ctx", None)),
        out_specs=P(("ctx", "head"), None),
        check_vma=False,
    )
```

```python
import functools
import math

import jax
import jax.numpy as jnp
from jax import lax
from jax.experimental import pallas as pl
from jax.experimental.pallas import tpu as pltpu
from jax.sharding import PartitionSpec as P

HDIM = 128
TILE = 128
MESH = pl.DeviceIdType.MESH
MASKED = -1e30
EXP2_SCALE = HDIM ** -0.5 / math.log(2.0)


def attend(tiles_ref, qb, work, sc, ob, j, t, base, own):
    slots = tiles_ref.shape[2]
    query = qb[j, t]
    ids, bias = [], []
    for s in range(slots):
        listed = tiles_ref[j, t, s]
        live = listed >= 0
        ids.append(jnp.clip(jnp.where(live, listed - base, own), 0, 3 * own - 1))
        bias.append(jnp.where(live, 0.0, MASKED))
    top = None
    for s in range(0, slots, 2):
        keys = jnp.concatenate([work[0, ids[s]], work[0, ids[s + 1]]], axis=0)
        scores = lax.dot_general(query, keys, (((1,), (1,)), ((), ())), preferred_element_type=jnp.float32)
        first = scores[:, :TILE] + bias[s]
        second = scores[:, TILE:] + bias[s + 1]
        sc[s] = first
        sc[s + 1] = second
        pair = jnp.maximum(first, second)
        top = pair if top is None else jnp.maximum(top, pair)
    row_max = jnp.max(top, axis=1, keepdims=True)
    total, numerator = None, None
    for s in range(0, slots, 2):
        first = jnp.exp2((sc[s] - row_max) * EXP2_SCALE)
        second = jnp.exp2((sc[s + 1] - row_max) * EXP2_SCALE)
        pair = first + second
        total = pair if total is None else total + pair
        probs = jnp.concatenate([first.astype(jnp.bfloat16), second.astype(jnp.bfloat16)], axis=1)
        values = jnp.concatenate([work[1, ids[s]], work[1, ids[s + 1]]], axis=0)
        part = jnp.dot(probs, values, preferred_element_type=jnp.float32)
        numerator = part if numerator is None else numerator + part
    row_total = jnp.sum(total, axis=1, keepdims=True)
    ob[j, t] = (numerator / row_total).astype(jnp.bfloat16)


def kernel(n_ctx, n_head, tiles_ref, q_ref, k_ref, v_ref, out_ref, qb, kvb, ob, work, sc, send_in, send_across_sem, send_halo, send_out, recv_kv, recv_q, recv_below, recv_above, recv_out):
    heads = tiles_ref.shape[0]
    c, me = lax.axis_index("ctx"), lax.axis_index("head")
    base = (c - 1) * n_head
    turn, last = n_ctx // 2, n_ctx - 1
    own, above = n_head, 2 * n_head
    at_end, at_turn = (c == 0) | (c == last), (c == turn - 1) | (c == turn)

    def columns(group, j):
        return pl.ds(pl.multiple_of((group * heads + j) * HDIM, HDIM), HDIM)

    def greet(ctx, head):
        pl.semaphore_signal(barrier, inc=1, device_id=(ctx, head), device_id_type=MESH)

    barrier = pltpu.get_barrier_semaphore()
    for p in range(1, n_head):
        greet(c, lax.rem(me + p, n_head))
    pl.when((c != 0) & (c != turn))(lambda: greet(c - 1, me))
    pl.when((c != last) & (c != turn - 1))(lambda: greet(c + 1, me))

    @pl.when(at_turn)
    def _():
        for group in range(n_head):
            greet(2 * turn - 1 - c, group)

    pl.semaphore_wait(barrier, jnp.where(at_end, n_head, jnp.where(at_turn, 2 * n_head, n_head + 1)))

    def send_tile(source, place, j, sem_index, recv):
        for p in range(1, n_head):
            peer = lax.rem(me + p, n_head)
            pltpu.make_async_remote_copy(
                src_ref=source.at[:, columns(peer, j)], dst_ref=place(), send_sem=send_in.at[sem_index],
                recv_sem=recv, device_id=(c, peer), device_id_type=MESH,
            ).start()
        pltpu.make_async_copy(source.at[:, columns(me, j)], place(), recv).start()

    def send_across(j, ctx, first, recv):
        for i, source in enumerate((k_ref, v_ref)):
            for p in range(n_head):
                group = lax.rem(me + p, n_head)
                pltpu.make_async_remote_copy(
                    src_ref=source.at[:, columns(group, j)], dst_ref=kvb.at[j, i, first + me], send_sem=send_across_sem.at[i],
                    recv_sem=recv.at[j], device_id=(ctx, group), device_id_type=MESH,
                ).start()

    def send_kv(j):
        send_tile(k_ref, lambda: kvb.at[j, 0, n_head + me], j, 0, recv_kv.at[j])
        send_tile(v_ref, lambda: kvb.at[j, 1, n_head + me], j, 1, recv_kv.at[j])
        pl.when(c == turn - 1)(lambda: send_across(j, turn, 0, recv_below))
        pl.when(c == turn)(lambda: send_across(j, turn - 1, above, recv_above))

    def send_q(j):
        send_tile(q_ref, lambda: qb.at[j, me], j, 2, recv_q.at[j])

    send_kv(0)

    @pl.loop(0, heads)
    def _(j):
        @pl.when(j + 1 < heads)
        def _():
            send_kv(j + 1)

        send_q(j)

    def push(j, source, place, count, ctx, recv):
        pltpu.make_async_remote_copy(
            src_ref=kvb.at[j, :, pl.ds(source, count)], dst_ref=kvb.at[j, :, pl.ds(place, count)],
            send_sem=send_halo, recv_sem=recv.at[j], device_id=(ctx, me), device_id_type=MESH,
        ).start()

    def landed(j, first, recv):
        slab = kvb.at[j, :, pl.ds(first, n_head)]
        pltpu.make_async_copy(slab, slab, recv.at[j]).wait()

    def pass_halo(j):
        landed(j, own, recv_kv)
        pl.when((c != 0) & (c != turn))(lambda: push(j, own, above, n_head, c - 1, recv_above))
        pl.when((c != last) & (c != turn - 1))(lambda: push(j, own, 0, n_head, c + 1, recv_below))

    def return_tile(j, t):
        place = out_ref.at[:, columns(me, j)]

        @pl.when(t == me)
        def _():
            pltpu.make_async_copy(ob.at[j, t], place, recv_out).start()

        @pl.when(t != me)
        def _():
            pltpu.make_async_remote_copy(
                src_ref=ob.at[j, t], dst_ref=place, send_sem=send_out,
                recv_sem=recv_out, device_id=(c, t), device_id_type=MESH,
            ).start()

    pass_halo(0)

    @pl.loop(0, heads)
    def _(j):
        @pl.when(j + 1 < heads)
        def _():
            pass_halo(j + 1)

        pl.when(c != 0)(lambda: landed(j, 0, recv_below))
        pl.when(c != last)(lambda: landed(j, above, recv_above))
        pltpu.make_async_copy(qb.at[j], qb.at[j], recv_q.at[j]).wait()

        @pl.loop(0, 3 * n_head)
        def _(i):
            work[0, i] = kvb[j, 0, i]
            work[1, i] = kvb[j, 1, i]

        @pl.loop(0, n_head)
        def _(i):
            t = lax.rem(me + 1 + i, n_head)
            attend(tiles_ref, qb, work, sc, ob, j, t, base, n_head)

            @pl.when(i > 0)
            def _():
                return_tile(j, lax.rem(me + i, n_head))

        return_tile(j, me)

    sent = qb.at[:, pl.ds(0, n_head - 1)]
    for i in range(3):
        pltpu.make_async_copy(sent, sent, send_in.at[i]).wait()
    halo = kvb.at[:, :, pl.ds(0, n_head)]
    pltpu.make_async_copy(halo, halo, send_halo).wait()
    pl.when(~(at_end | at_turn))(lambda: pltpu.make_async_copy(halo, halo, send_halo).wait())

    @pl.when(at_turn)
    def _():
        for i in range(2):
            pltpu.make_async_copy(qb, qb, send_across_sem.at[i]).wait()

    pltpu.make_async_copy(sent, sent, send_out).wait()
    pltpu.make_async_copy(out_ref, out_ref, recv_out).wait()


def solution(mesh):
    n_ctx, n_head = mesh.shape["ctx"], mesh.shape["head"]

    def shards(queries, key_rows, value_rows, key_tiles):
        heads, _, slots = key_tiles.shape
        return pl.pallas_call(
            functools.partial(kernel, n_ctx, n_head),
            out_shape=jax.ShapeDtypeStruct(queries.shape, queries.dtype),
            in_specs=[pl.BlockSpec(memory_space=pltpu.SMEM)] + [pl.BlockSpec(memory_space=pltpu.HBM)] * 3,
            out_specs=pl.BlockSpec(memory_space=pltpu.HBM),
            scratch_shapes=[
                pltpu.VMEM((heads, n_head, TILE, HDIM), jnp.bfloat16),
                pltpu.VMEM((heads, 2, 3 * n_head, TILE, HDIM), jnp.bfloat16),
                pltpu.VMEM((heads, n_head, TILE, HDIM), jnp.bfloat16),
                pltpu.VMEM((2, 3 * n_head, TILE, HDIM), jnp.bfloat16),
                pltpu.VMEM((slots, TILE, TILE), jnp.float32),
                pltpu.SemaphoreType.DMA((3,)),
                pltpu.SemaphoreType.DMA((2,)),
                pltpu.SemaphoreType.DMA,
                pltpu.SemaphoreType.DMA,
                pltpu.SemaphoreType.DMA((heads,)),
                pltpu.SemaphoreType.DMA((heads,)),
                pltpu.SemaphoreType.DMA((heads,)),
                pltpu.SemaphoreType.DMA((heads,)),
                pltpu.SemaphoreType.DMA,
            ],
            compiler_params=pltpu.CompilerParams(
                collective_id=0, has_side_effects=True, vmem_limit_bytes=67043328
            ),
        )(key_tiles, queries, key_rows, value_rows)

    return jax.shard_map(
        shards,
        mesh=mesh,
        in_specs=(P(("ctx", "head"), None), P(("ctx", "head"), None), P(("ctx", "head"), None), P("head", "ctx", None)),
        out_specs=P(("ctx", "head"), None),
        check_vma=False,
    )
```

```python
import functools
import math

import jax
import jax.numpy as jnp
from jax import lax
from jax.experimental import pallas as pl
from jax.experimental.pallas import tpu as pltpu
from jax.sharding import PartitionSpec as P

HDIM = 128
TILE = 128
MESH = pl.DeviceIdType.MESH
MASKED = -1e30
EXP2_SCALE = HDIM ** -0.5 / math.log(2.0)


def listed_tiles(tiles_ref, j, t, base, own):
    ids, bias = [], []
    for s in range(tiles_ref.shape[2]):
        listed = tiles_ref[j, t, s]
        live = listed >= 0
        ids.append(jnp.clip(jnp.where(live, listed - base, own + t), 0, 3 * own - 1))
        bias.append(jnp.where(live, 0.0, MASKED))
    return ids, bias


def score(qb, work, sc, ids, j, t):
    query = qb[j, t]
    top = None
    for s in range(0, len(ids), 2):
        keys = jnp.concatenate([work[0, ids[s]], work[0, ids[s + 1]]], axis=0)
        scores = lax.dot_general(query, keys, (((1,), (1,)), ((), ())), preferred_element_type=jnp.float32)
        sc[s] = scores[:, :TILE]
        sc[s + 1] = scores[:, TILE:]
        pair = jnp.maximum(scores[:, :TILE], scores[:, TILE:])
        top = pair if top is None else jnp.maximum(top, pair)
    return jnp.max(top, axis=1, keepdims=True)


def gather(work, sc, pb, ob, ids, bias, row_max, j, t):
    total, numerator = None, None
    for s in range(0, len(ids), 2):
        first = jnp.exp2((sc[s] - row_max) * EXP2_SCALE + bias[s])
        second = jnp.exp2((sc[s + 1] - row_max) * EXP2_SCALE + bias[s + 1])
        pair = first + second
        total = pair if total is None else total + pair
        probs = jnp.concatenate([first.astype(jnp.bfloat16), second.astype(jnp.bfloat16)], axis=1)
        values = jnp.concatenate([work[1, ids[s]], work[1, ids[s + 1]]], axis=0)
        part = jnp.dot(probs, values, preferred_element_type=jnp.float32)
        numerator = part if numerator is None else numerator + part
    row_total = jnp.sum(total, axis=1, keepdims=True)
    ob[j, t] = (numerator / row_total).astype(jnp.bfloat16)


def kernel(n_ctx, n_head, tiles_ref, q_ref, k_ref, v_ref, out_ref, qb, kvb, ob, work, sc, pb, send_in, send_across_sem, send_halo, send_out, recv_kv, recv_q, recv_below, recv_above, recv_out):
    heads = tiles_ref.shape[0]
    c, me = lax.axis_index("ctx"), lax.axis_index("head")
    base = (c - 1) * n_head
    turn, last = n_ctx // 2, n_ctx - 1
    own, above = n_head, 2 * n_head
    at_end, at_turn = (c == 0) | (c == last), (c == turn - 1) | (c == turn)

    def columns(group, j):
        return pl.ds(pl.multiple_of((group * heads + j) * HDIM, HDIM), HDIM)

    def greet(ctx, head):
        pl.semaphore_signal(barrier, inc=1, device_id=(ctx, head), device_id_type=MESH)

    barrier = pltpu.get_barrier_semaphore()
    for p in range(1, n_head):
        greet(c, lax.rem(me + p, n_head))
    pl.when((c != 0) & (c != turn))(lambda: greet(c - 1, me))
    pl.when((c != last) & (c != turn - 1))(lambda: greet(c + 1, me))

    @pl.when(at_turn)
    def _():
        for group in range(n_head):
            greet(2 * turn - 1 - c, group)

    pl.semaphore_wait(barrier, jnp.where(at_end, n_head, jnp.where(at_turn, 2 * n_head, n_head + 1)))

    def send_tile(source, place, j, sem_index, recv):
        for p in range(1, n_head):
            peer = lax.rem(me + p, n_head)
            pltpu.make_async_remote_copy(
                src_ref=source.at[:, columns(peer, j)], dst_ref=place(), send_sem=send_in.at[sem_index],
                recv_sem=recv, device_id=(c, peer), device_id_type=MESH,
            ).start()
        pltpu.make_async_copy(source.at[:, columns(me, j)], place(), recv).start()

    def send_across(j, ctx, first, recv):
        for i, source in enumerate((k_ref, v_ref)):
            for p in range(n_head):
                group = lax.rem(me + p, n_head)
                pltpu.make_async_remote_copy(
                    src_ref=source.at[:, columns(group, j)], dst_ref=kvb.at[j, i, first + me], send_sem=send_across_sem.at[i],
                    recv_sem=recv.at[j], device_id=(ctx, group), device_id_type=MESH,
                ).start()

    def send_kv(j):
        send_tile(k_ref, lambda: kvb.at[j, 0, n_head + me], j, 0, recv_kv.at[j])
        send_tile(v_ref, lambda: kvb.at[j, 1, n_head + me], j, 1, recv_kv.at[j])
        pl.when(c == turn - 1)(lambda: send_across(j, turn, 0, recv_below))
        pl.when(c == turn)(lambda: send_across(j, turn - 1, above, recv_above))

    def send_q(j):
        send_tile(q_ref, lambda: qb.at[j, me], j, 2, recv_q.at[j])

    send_kv(0)

    @pl.loop(0, heads)
    def _(j):
        @pl.when(j + 1 < heads)
        def _():
            send_kv(j + 1)

        send_q(j)

    def push(j, source, place, count, ctx, recv):
        pltpu.make_async_remote_copy(
            src_ref=kvb.at[j, :, pl.ds(source, count)], dst_ref=kvb.at[j, :, pl.ds(place, count)],
            send_sem=send_halo, recv_sem=recv.at[j], device_id=(ctx, me), device_id_type=MESH,
        ).start()

    def landed(j, first, recv):
        slab = kvb.at[j, :, pl.ds(first, n_head)]
        pltpu.make_async_copy(slab, slab, recv.at[j]).wait()

    def pass_halo(j):
        landed(j, own, recv_kv)
        pl.when((c != 0) & (c != turn))(lambda: push(j, own, above, n_head, c - 1, recv_above))
        pl.when((c != last) & (c != turn - 1))(lambda: push(j, own, 0, n_head, c + 1, recv_below))

    def return_tile(j, t):
        place = out_ref.at[:, columns(me, j)]

        @pl.when(t == me)
        def _():
            pltpu.make_async_copy(ob.at[j, t], place, recv_out).start()

        @pl.when(t != me)
        def _():
            pltpu.make_async_remote_copy(
                src_ref=ob.at[j, t], dst_ref=place, send_sem=send_out,
                recv_sem=recv_out, device_id=(c, t), device_id_type=MESH,
            ).start()

    pass_halo(0)

    @pl.loop(0, heads)
    def _(j):
        @pl.when(j + 1 < heads)
        def _():
            pass_halo(j + 1)

        pl.when(c != 0)(lambda: landed(j, 0, recv_below))
        pl.when(c != last)(lambda: landed(j, above, recv_above))
        pltpu.make_async_copy(qb.at[j], qb.at[j], recv_q.at[j]).wait()

        @pl.loop(0, 3 * n_head)
        def _(i):
            work[0, i] = kvb[j, 0, i]
            work[1, i] = kvb[j, 1, i]

        @pl.loop(0, n_head, step=2)
        def _(i):
            tiles = [lax.rem(me + 1 + i + k, n_head) for k in range(2)]
            lists = [listed_tiles(tiles_ref, j, t, base, n_head) for t in tiles]
            tops = [score(qb, work, sc.at[k], lists[k][0], j, tiles[k]) for k in range(2)]
            for k in range(2):
                gather(work, sc.at[k], pb.at[k], ob, *lists[k], tops[k], j, tiles[k])

            @pl.when(i > 0)
            def _():
                for k in range(2):
                    return_tile(j, lax.rem(me - 1 + i + k, n_head))

        return_tile(j, lax.rem(me + n_head - 1, n_head))
        return_tile(j, me)

    sent = qb.at[:, pl.ds(0, n_head - 1)]
    for i in range(3):
        pltpu.make_async_copy(sent, sent, send_in.at[i]).wait()
    halo = kvb.at[:, :, pl.ds(0, n_head)]
    pltpu.make_async_copy(halo, halo, send_halo).wait()
    pl.when(~(at_end | at_turn))(lambda: pltpu.make_async_copy(halo, halo, send_halo).wait())

    @pl.when(at_turn)
    def _():
        for i in range(2):
            pltpu.make_async_copy(qb, qb, send_across_sem.at[i]).wait()

    pltpu.make_async_copy(sent, sent, send_out).wait()
    pltpu.make_async_copy(out_ref, out_ref, recv_out).wait()


def solution(mesh):
    n_ctx, n_head = mesh.shape["ctx"], mesh.shape["head"]

    def shards(queries, key_rows, value_rows, key_tiles):
        heads, _, slots = key_tiles.shape
        return pl.pallas_call(
            functools.partial(kernel, n_ctx, n_head),
            out_shape=jax.ShapeDtypeStruct(queries.shape, queries.dtype),
            in_specs=[pl.BlockSpec(memory_space=pltpu.SMEM)] + [pl.BlockSpec(memory_space=pltpu.HBM)] * 3,
            out_specs=pl.BlockSpec(memory_space=pltpu.HBM),
            scratch_shapes=[
                pltpu.VMEM((heads, n_head, TILE, HDIM), jnp.bfloat16),
                pltpu.VMEM((heads, 2, 3 * n_head, TILE, HDIM), jnp.bfloat16),
                pltpu.VMEM((heads, n_head, TILE, HDIM), jnp.bfloat16),
                pltpu.VMEM((2, 3 * n_head, TILE, HDIM), jnp.bfloat16),
                pltpu.VMEM((2, slots, TILE, TILE), jnp.float32),
                pltpu.VMEM((2, TILE, slots * TILE), jnp.bfloat16),
                pltpu.SemaphoreType.DMA((3,)),
                pltpu.SemaphoreType.DMA((2,)),
                pltpu.SemaphoreType.DMA,
                pltpu.SemaphoreType.DMA,
                pltpu.SemaphoreType.DMA((heads,)),
                pltpu.SemaphoreType.DMA((heads,)),
                pltpu.SemaphoreType.DMA((heads,)),
                pltpu.SemaphoreType.DMA((heads,)),
                pltpu.SemaphoreType.DMA,
            ],
            compiler_params=pltpu.CompilerParams(
                collective_id=0, has_side_effects=True, vmem_limit_bytes=67043328
            ),
        )(key_tiles, queries, key_rows, value_rows)

    return jax.shard_map(
        shards,
        mesh=mesh,
        in_specs=(P(("ctx", "head"), None), P(("ctx", "head"), None), P(("ctx", "head"), None), P("head", "ctx", None)),
        out_specs=P(("ctx", "head"), None),
        check_vma=False,
    )
```

```python
import functools
import math

import jax
import jax.numpy as jnp
from jax import lax
from jax.experimental import pallas as pl
from jax.experimental.pallas import tpu as pltpu
from jax.sharding import PartitionSpec as P

HDIM = 128
TILE = 128
MESH = pl.DeviceIdType.MESH
MASKED = -1e30
EXP2_SCALE = HDIM ** -0.5 / math.log(2.0)


def listed_tiles(tiles_ref, j, t, base, own):
    ids, bias = [], []
    for s in range(tiles_ref.shape[2]):
        listed = tiles_ref[j, t, s]
        live = listed >= 0
        ids.append(jnp.clip(jnp.where(live, listed - base, own + t), 0, 3 * own - 1))
        bias.append(jnp.where(live, 0.0, MASKED))
    return ids, bias


def score(qb, work, sc, ids, j, t):
    query = qb[j, t]
    top = None
    for s in range(0, len(ids), 2):
        keys = jnp.concatenate([work[0, ids[s]], work[0, ids[s + 1]]], axis=0)
        scores = lax.dot_general(query, keys, (((1,), (1,)), ((), ())), preferred_element_type=jnp.float32)
        sc[s] = scores[:, :TILE]
        sc[s + 1] = scores[:, TILE:]
        pair = jnp.maximum(scores[:, :TILE], scores[:, TILE:])
        top = pair if top is None else jnp.maximum(top, pair)
    return jnp.max(top, axis=1, keepdims=True)


def gather(work, sc, ob, ids, bias, row_max, j, t):
    total, numerator = None, None
    for s in range(0, len(ids), 2):
        first = jnp.exp2((sc[s] - row_max) * EXP2_SCALE + bias[s])
        second = jnp.exp2((sc[s + 1] - row_max) * EXP2_SCALE + bias[s + 1])
        pair = first + second
        total = pair if total is None else total + pair
        probs = jnp.concatenate([first.astype(jnp.bfloat16), second.astype(jnp.bfloat16)], axis=1)
        values = jnp.concatenate([work[1, ids[s]], work[1, ids[s + 1]]], axis=0)
        part = jnp.dot(probs, values, preferred_element_type=jnp.float32)
        numerator = part if numerator is None else numerator + part
    row_total = jnp.sum(total, axis=1, keepdims=True)
    ob[j, t] = (numerator / row_total).astype(jnp.bfloat16)


def kernel(n_ctx, n_head, tiles_ref, q_ref, k_ref, v_ref, out_ref, qb, kvb, passing, ob, work, sc, send_in, send_across_sem, send_halo, send_passing, send_out, recv_kv, recv_q, recv_below, recv_above, recv_passing, recv_out):
    heads = tiles_ref.shape[0]
    c, me = lax.axis_index("ctx"), lax.axis_index("head")
    base = (c - 1) * n_head
    turn, last = n_ctx // 2, n_ctx - 1
    own, above, part = n_head, 2 * n_head, n_head // 2
    via = ((turn // 2 - 1, 0), (turn // 2, part))
    at_end, at_turn = (c == 0) | (c == last), (c == turn - 1) | (c == turn)
    at_via = functools.reduce(jnp.logical_or, [c == plane + place for plane in (0, turn) for place, _ in via])
    far_plane = jnp.where(c < turn, turn, 0)

    def columns(group, j):
        return pl.ds(pl.multiple_of((group * heads + j) * HDIM, HDIM), HDIM)

    def greet(ctx, head):
        pl.semaphore_signal(barrier, inc=1, device_id=(ctx, head), device_id_type=MESH)

    barrier = pltpu.get_barrier_semaphore()
    for p in range(1, n_head):
        greet(c, lax.rem(me + p, n_head))
    pl.when((c != 0) & (c != turn))(lambda: greet(c - 1, me))
    pl.when((c != last) & (c != turn - 1))(lambda: greet(c + 1, me))

    @pl.when(at_turn)
    def _():
        for group in range(n_head):
            greet(2 * turn - 1 - c, group)
        for place, _ in via:
            greet(place, me)
            greet(turn + place, me)

    @pl.when(at_via)
    def _():
        greet(turn - 1, me)
        greet(turn, me)

    greeted = jnp.where(at_end, n_head, jnp.where(at_turn, 2 * n_head + 4, jnp.where(at_via, n_head + 3, n_head + 1)))
    pl.semaphore_wait(barrier, greeted)

    def send_tile(source, place, j, sem_index, recv):
        for p in range(1, n_head):
            peer = lax.rem(me + p, n_head)
            pltpu.make_async_remote_copy(
                src_ref=source.at[:, columns(peer, j)], dst_ref=place(), send_sem=send_in.at[sem_index],
                recv_sem=recv, device_id=(c, peer), device_id_type=MESH,
            ).start()
        pltpu.make_async_copy(source.at[:, columns(me, j)], place(), recv).start()

    def send_across(j, ctx, first, recv):
        for p in range(n_head):
            group = lax.rem(me + p, n_head)
            pltpu.make_async_remote_copy(
                src_ref=k_ref.at[:, columns(group, j)], dst_ref=kvb.at[j, 0, first + me], send_sem=send_across_sem,
                recv_sem=recv.at[j], device_id=(ctx, group), device_id_type=MESH,
            ).start()

    def send_kv(j):
        send_tile(k_ref, lambda: kvb.at[j, 0, n_head + me], j, 0, recv_kv.at[j])
        send_tile(v_ref, lambda: kvb.at[j, 1, n_head + me], j, 1, recv_kv.at[j])
        pl.when(c == turn - 1)(lambda: send_across(j, turn, 0, recv_below))
        pl.when(c == turn)(lambda: send_across(j, turn - 1, above, recv_above))

    def send_q(j):
        send_tile(q_ref, lambda: qb.at[j, me], j, 2, recv_q.at[j])

    send_kv(0)

    @pl.loop(0, heads)
    def _(j):
        @pl.when(j + 1 < heads)
        def _():
            send_kv(j + 1)

        send_q(j)

    def push(j, source, place, count, ctx, recv):
        pltpu.make_async_remote_copy(
            src_ref=kvb.at[j, :, pl.ds(source, count)], dst_ref=kvb.at[j, :, pl.ds(place, count)],
            send_sem=send_halo, recv_sem=recv.at[j], device_id=(ctx, me), device_id_type=MESH,
        ).start()

    def landed(j, first, recv):
        slab = kvb.at[j, :, pl.ds(first, n_head)]
        pltpu.make_async_copy(slab, slab, recv.at[j]).wait()

    def pass_halo(j):
        landed(j, own, recv_kv)

        @pl.when(at_turn)
        def _():
            for place, first in via:
                pltpu.make_async_remote_copy(
                    src_ref=kvb.at[j, 1, pl.ds(own + first, part)], dst_ref=passing.at[j], send_sem=send_halo,
                    recv_sem=recv_passing.at[j], device_id=(far_plane + place, me), device_id_type=MESH,
                ).start()

        pl.when((c != 0) & (c != turn))(lambda: push(j, own, above, n_head, c - 1, recv_above))
        pl.when((c != last) & (c != turn - 1))(lambda: push(j, own, 0, n_head, c + 1, recv_below))

    def relay(j):
        for plane, target, shift, recv in ((0, turn - 1, above, recv_above), (turn, turn, 0, recv_below)):
            for place, first in via:
                @pl.when(c == plane + place)
                def _():
                    pltpu.make_async_copy(passing.at[j], passing.at[j], recv_passing.at[j]).wait()
                    pltpu.make_async_remote_copy(
                        src_ref=passing.at[j], dst_ref=kvb.at[j, 1, pl.ds(shift + first, part)], send_sem=send_passing,
                        recv_sem=recv.at[j], device_id=(target, me), device_id_type=MESH,
                    ).start()

    def return_tile(j, t):
        place = out_ref.at[:, columns(me, j)]

        @pl.when(t == me)
        def _():
            pltpu.make_async_copy(ob.at[j, t], place, recv_out).start()

        @pl.when(t != me)
        def _():
            pltpu.make_async_remote_copy(
                src_ref=ob.at[j, t], dst_ref=place, send_sem=send_out,
                recv_sem=recv_out, device_id=(c, t), device_id_type=MESH,
            ).start()

    pass_halo(0)
    relay(0)

    @pl.loop(0, heads)
    def _(j):
        @pl.when(j + 1 < heads)
        def _():
            pass_halo(j + 1)

        pl.when(c != 0)(lambda: landed(j, 0, recv_below))
        pl.when(c != last)(lambda: landed(j, above, recv_above))
        pltpu.make_async_copy(qb.at[j], qb.at[j], recv_q.at[j]).wait()

        @pl.loop(0, 3 * n_head)
        def _(i):
            work[0, i] = kvb[j, 0, i]
            work[1, i] = kvb[j, 1, i]

        @pl.loop(0, n_head, step=2)
        def _(i):
            tiles = [lax.rem(me + 1 + i + k, n_head) for k in range(2)]
            lists = [listed_tiles(tiles_ref, j, t, base, n_head) for t in tiles]
            tops = [score(qb, work, sc.at[k], lists[k][0], j, tiles[k]) for k in range(2)]
            for k in range(2):
                gather(work, sc.at[k], ob, *lists[k], tops[k], j, tiles[k])

            @pl.when((i == 4) & (j + 1 < heads))
            def _():
                relay(j + 1)

            @pl.when(i > 0)
            def _():
                for k in range(2):
                    return_tile(j, lax.rem(me - 1 + i + k, n_head))

        return_tile(j, lax.rem(me + n_head - 1, n_head))
        return_tile(j, me)

    sent = qb.at[:, pl.ds(0, n_head - 1)]
    for i in range(3):
        pltpu.make_async_copy(sent, sent, send_in.at[i]).wait()
    halo, half = kvb.at[:, :, pl.ds(0, n_head)], kvb.at[:, 0, pl.ds(0, n_head)]
    pltpu.make_async_copy(halo, halo, send_halo).wait()
    pl.when(~(at_end | at_turn))(lambda: pltpu.make_async_copy(halo, halo, send_halo).wait())

    @pl.when(at_turn)
    def _():
        pltpu.make_async_copy(half, half, send_halo).wait()
        pltpu.make_async_copy(qb, qb, send_across_sem).wait()

    pl.when(at_via)(lambda: pltpu.make_async_copy(passing, passing, send_passing).wait())
    pltpu.make_async_copy(sent, sent, send_out).wait()
    pltpu.make_async_copy(out_ref, out_ref, recv_out).wait()


def solution(mesh):
    n_ctx, n_head = mesh.shape["ctx"], mesh.shape["head"]

    def shards(queries, key_rows, value_rows, key_tiles):
        heads, _, slots = key_tiles.shape
        return pl.pallas_call(
            functools.partial(kernel, n_ctx, n_head),
            out_shape=jax.ShapeDtypeStruct(queries.shape, queries.dtype),
            in_specs=[pl.BlockSpec(memory_space=pltpu.SMEM)] + [pl.BlockSpec(memory_space=pltpu.HBM)] * 3,
            out_specs=pl.BlockSpec(memory_space=pltpu.HBM),
            scratch_shapes=[
                pltpu.VMEM((heads, n_head, TILE, HDIM), jnp.bfloat16),
                pltpu.VMEM((heads, 2, 3 * n_head, TILE, HDIM), jnp.bfloat16),
                pltpu.VMEM((heads, n_head // 2, TILE, HDIM), jnp.bfloat16),
                pltpu.VMEM((heads, n_head, TILE, HDIM), jnp.bfloat16),
                pltpu.VMEM((2, 3 * n_head, TILE, HDIM), jnp.bfloat16),
                pltpu.VMEM((2, slots, TILE, TILE), jnp.float32),
                pltpu.SemaphoreType.DMA((3,)),
                pltpu.SemaphoreType.DMA,
                pltpu.SemaphoreType.DMA,
                pltpu.SemaphoreType.DMA,
                pltpu.SemaphoreType.DMA,
                pltpu.SemaphoreType.DMA((heads,)),
                pltpu.SemaphoreType.DMA((heads,)),
                pltpu.SemaphoreType.DMA((heads,)),
                pltpu.SemaphoreType.DMA((heads,)),
                pltpu.SemaphoreType.DMA((heads,)),
                pltpu.SemaphoreType.DMA,
            ],
            compiler_params=pltpu.CompilerParams(
                collective_id=0, has_side_effects=True, vmem_limit_bytes=67043328
            ),
        )(key_tiles, queries, key_rows, value_rows)

    return jax.shard_map(
        shards,
        mesh=mesh,
        in_specs=(P(("ctx", "head"), None), P(("ctx", "head"), None), P(("ctx", "head"), None), P("head", "ctx", None)),
        out_specs=P(("ctx", "head"), None),
        check_vma=False,
    )
```

```python
import functools
import math

import jax
import jax.numpy as jnp
from jax import lax
from jax.experimental import pallas as pl
from jax.experimental.pallas import tpu as pltpu
from jax.sharding import PartitionSpec as P

HDIM = 128
TILE = 128
MESH = pl.DeviceIdType.MESH
MASKED = -1e30
EXP2_SCALE = HDIM ** -0.5 / math.log(2.0)


def listed_tiles(tiles_ref, j, t, base, own):
    ids, bias = [], []
    for s in range(tiles_ref.shape[2]):
        listed = tiles_ref[j, t, s]
        live = listed >= 0
        ids.append(jnp.clip(jnp.where(live, listed - base, own + t), 0, 3 * own - 1))
        bias.append(jnp.where(live, 0.0, MASKED))
    return ids, bias


def score(qb, work, sc, ids, j, t):
    query = qb[j, t]
    top = None
    for s in range(0, len(ids), 2):
        keys = jnp.concatenate([work[0, ids[s]], work[0, ids[s + 1]]], axis=0)
        scores = lax.dot_general(query, keys, (((1,), (1,)), ((), ())), preferred_element_type=jnp.float32)
        sc[s] = scores[:, :TILE]
        sc[s + 1] = scores[:, TILE:]
        pair = jnp.maximum(scores[:, :TILE], scores[:, TILE:])
        top = pair if top is None else jnp.maximum(top, pair)
    return jnp.max(top, axis=1, keepdims=True)


def gather(work, sc, ob, ids, bias, row_max, j, t):
    total, numerator = None, None
    for s in range(0, len(ids), 2):
        first = jnp.exp2((sc[s] - row_max) * EXP2_SCALE + bias[s])
        second = jnp.exp2((sc[s + 1] - row_max) * EXP2_SCALE + bias[s + 1])
        pair = first + second
        total = pair if total is None else total + pair
        probs = jnp.concatenate([first.astype(jnp.bfloat16), second.astype(jnp.bfloat16)], axis=1)
        values = jnp.concatenate([work[1, ids[s]], work[1, ids[s + 1]]], axis=0)
        part = jnp.dot(probs, values, preferred_element_type=jnp.float32)
        numerator = part if numerator is None else numerator + part
    row_total = jnp.sum(total, axis=1, keepdims=True)
    ob[j, t] = (numerator / row_total).astype(jnp.bfloat16)


def kernel(n_ctx, n_head, tiles_ref, q_ref, k_ref, v_ref, out_ref, qb, kvb, passing, ob, work, sc, send_in, send_across_sem, send_halo, send_passing, send_out, recv_kv, recv_q, recv_below, recv_above, recv_passing, recv_out):
    heads = tiles_ref.shape[0]
    c, me = lax.axis_index("ctx"), lax.axis_index("head")
    base = (c - 1) * n_head
    turn, last = n_ctx // 2, n_ctx - 1
    own, above, part = n_head, 2 * n_head, n_head // 2
    via = ((turn // 2 - 1, 0), (turn // 2, part))
    at_end, at_turn = (c == 0) | (c == last), (c == turn - 1) | (c == turn)
    at_via = functools.reduce(jnp.logical_or, [c == plane + place for plane in (0, turn) for place, _ in via])
    far_plane = jnp.where(c < turn, turn, 0)

    def columns(group, j):
        return pl.ds(pl.multiple_of((group * heads + j) * HDIM, HDIM), HDIM)

    def greet(ctx, head):
        pl.semaphore_signal(barrier, inc=1, device_id=(ctx, head), device_id_type=MESH)

    barrier = pltpu.get_barrier_semaphore()
    for p in range(1, n_head):
        greet(c, lax.rem(me + p, n_head))
    pl.when((c != 0) & (c != turn))(lambda: greet(c - 1, me))
    pl.when((c != last) & (c != turn - 1))(lambda: greet(c + 1, me))

    @pl.when(at_turn)
    def _():
        for group in range(n_head):
            greet(2 * turn - 1 - c, group)
        for place, _ in via:
            greet(place, me)
            greet(turn + place, me)

    @pl.when(at_via)
    def _():
        greet(turn - 1, me)
        greet(turn, me)

    greeted = jnp.where(at_end, n_head, jnp.where(at_turn, 2 * n_head + 4, jnp.where(at_via, n_head + 3, n_head + 1)))
    pl.semaphore_wait(barrier, greeted)

    def send_tile(source, place, j, sem_index, recv):
        for p in range(1, n_head):
            peer = lax.rem(me + p, n_head)
            pltpu.make_async_remote_copy(
                src_ref=source.at[:, columns(peer, j)], dst_ref=place(), send_sem=send_in.at[sem_index],
                recv_sem=recv, device_id=(c, peer), device_id_type=MESH,
            ).start()
        pltpu.make_async_copy(source.at[:, columns(me, j)], place(), recv).start()

    def send_across(j, ctx, first, recv):
        for p in range(n_head):
            group = lax.rem(me + p, n_head)
            pltpu.make_async_remote_copy(
                src_ref=k_ref.at[:, columns(group, j)], dst_ref=kvb.at[j, 0, first + me], send_sem=send_across_sem,
                recv_sem=recv.at[j], device_id=(ctx, group), device_id_type=MESH,
            ).start()

    def send_kv(j):
        send_tile(k_ref, lambda: kvb.at[j, 0, n_head + me], j, 0, recv_kv.at[j])
        send_tile(v_ref, lambda: kvb.at[j, 1, n_head + me], j, 1, recv_kv.at[j])
        pl.when(c == turn - 1)(lambda: send_across(j, turn, 0, recv_below))
        pl.when(c == turn)(lambda: send_across(j, turn - 1, above, recv_above))

    def send_q(j):
        send_tile(q_ref, lambda: qb.at[j, me], j, 2, recv_q.at[j])

    send_kv(0)

    @pl.loop(0, heads)
    def _(j):
        @pl.when(j + 1 < heads)
        def _():
            send_kv(j + 1)

        send_q(j)

    def push(j, source, place, count, ctx, recv):
        pltpu.make_async_remote_copy(
            src_ref=kvb.at[j, :, pl.ds(source, count)], dst_ref=kvb.at[j, :, pl.ds(place, count)],
            send_sem=send_halo, recv_sem=recv.at[j], device_id=(ctx, me), device_id_type=MESH,
        ).start()

    def landed(j, first, recv):
        slab = kvb.at[j, :, pl.ds(first, n_head)]
        pltpu.make_async_copy(slab, slab, recv.at[j]).wait()

    def pass_halo(j):
        landed(j, own, recv_kv)

        @pl.when(at_turn)
        def _():
            for place, first in via:
                pltpu.make_async_remote_copy(
                    src_ref=kvb.at[j, 1, pl.ds(own + first, part)], dst_ref=passing.at[j], send_sem=send_halo,
                    recv_sem=recv_passing.at[j], device_id=(far_plane + place, me), device_id_type=MESH,
                ).start()

        pl.when((c != 0) & (c != turn))(lambda: push(j, own, above, n_head, c - 1, recv_above))
        pl.when((c != last) & (c != turn - 1))(lambda: push(j, own, 0, n_head, c + 1, recv_below))

    def relay(j):
        for plane, target, shift, recv in ((0, turn - 1, above, recv_above), (turn, turn, 0, recv_below)):
            for place, first in via:
                @pl.when(c == plane + place)
                def _():
                    pltpu.make_async_copy(passing.at[j], passing.at[j], recv_passing.at[j]).wait()
                    pltpu.make_async_remote_copy(
                        src_ref=passing.at[j], dst_ref=kvb.at[j, 1, pl.ds(shift + first, part)], send_sem=send_passing,
                        recv_sem=recv.at[j], device_id=(target, me), device_id_type=MESH,
                    ).start()

    def return_tile(j, t):
        place = out_ref.at[:, columns(me, j)]

        @pl.when(t == me)
        def _():
            pltpu.make_async_copy(ob.at[j, t], place, recv_out).start()

        @pl.when(t != me)
        def _():
            pltpu.make_async_remote_copy(
                src_ref=ob.at[j, t], dst_ref=place, send_sem=send_out,
                recv_sem=recv_out, device_id=(c, t), device_id_type=MESH,
            ).start()

    pass_halo(0)
    pass_halo(1)
    relay(0)

    @pl.loop(0, heads)
    def _(j):
        @pl.when(j + 2 < heads)
        def _():
            pass_halo(j + 2)

        pl.when(c != 0)(lambda: landed(j, 0, recv_below))
        pl.when(c != last)(lambda: landed(j, above, recv_above))
        pltpu.make_async_copy(qb.at[j], qb.at[j], recv_q.at[j]).wait()

        @pl.loop(0, 3 * n_head)
        def _(i):
            work[0, i] = kvb[j, 0, i]
            work[1, i] = kvb[j, 1, i]

        @pl.loop(0, n_head, step=2)
        def _(i):
            tiles = [lax.rem(me + 1 + i + k, n_head) for k in range(2)]
            lists = [listed_tiles(tiles_ref, j, t, base, n_head) for t in tiles]
            tops = [score(qb, work, sc.at[k], lists[k][0], j, tiles[k]) for k in range(2)]
            for k in range(2):
                gather(work, sc.at[k], ob, *lists[k], tops[k], j, tiles[k])

            @pl.when((i == 0) & (j + 1 < heads))
            def _():
                relay(j + 1)

            @pl.when(i > 0)
            def _():
                for k in range(2):
                    return_tile(j, lax.rem(me - 1 + i + k, n_head))

        return_tile(j, lax.rem(me + n_head - 1, n_head))
        return_tile(j, me)

    sent = qb.at[:, pl.ds(0, n_head - 1)]
    for i in range(3):
        pltpu.make_async_copy(sent, sent, send_in.at[i]).wait()
    halo, half = kvb.at[:, :, pl.ds(0, n_head)], kvb.at[:, 0, pl.ds(0, n_head)]
    pltpu.make_async_copy(halo, halo, send_halo).wait()
    pl.when(~(at_end | at_turn))(lambda: pltpu.make_async_copy(halo, halo, send_halo).wait())

    @pl.when(at_turn)
    def _():
        pltpu.make_async_copy(half, half, send_halo).wait()
        pltpu.make_async_copy(qb, qb, send_across_sem).wait()

    pl.when(at_via)(lambda: pltpu.make_async_copy(passing, passing, send_passing).wait())
    pltpu.make_async_copy(sent, sent, send_out).wait()
    pltpu.make_async_copy(out_ref, out_ref, recv_out).wait()


def solution(mesh):
    n_ctx, n_head = mesh.shape["ctx"], mesh.shape["head"]

    def shards(queries, key_rows, value_rows, key_tiles):
        heads, _, slots = key_tiles.shape
        return pl.pallas_call(
            functools.partial(kernel, n_ctx, n_head),
            out_shape=jax.ShapeDtypeStruct(queries.shape, queries.dtype),
            in_specs=[pl.BlockSpec(memory_space=pltpu.SMEM)] + [pl.BlockSpec(memory_space=pltpu.HBM)] * 3,
            out_specs=pl.BlockSpec(memory_space=pltpu.HBM),
            scratch_shapes=[
                pltpu.VMEM((heads, n_head, TILE, HDIM), jnp.bfloat16),
                pltpu.VMEM((heads, 2, 3 * n_head, TILE, HDIM), jnp.bfloat16),
                pltpu.VMEM((heads, n_head // 2, TILE, HDIM), jnp.bfloat16),
                pltpu.VMEM((heads, n_head, TILE, HDIM), jnp.bfloat16),
                pltpu.VMEM((2, 3 * n_head, TILE, HDIM), jnp.bfloat16),
                pltpu.VMEM((2, slots, TILE, TILE), jnp.float32),
                pltpu.SemaphoreType.DMA((3,)),
                pltpu.SemaphoreType.DMA,
                pltpu.SemaphoreType.DMA,
                pltpu.SemaphoreType.DMA,
                pltpu.SemaphoreType.DMA,
                pltpu.SemaphoreType.DMA((heads,)),
                pltpu.SemaphoreType.DMA((heads,)),
                pltpu.SemaphoreType.DMA((heads,)),
                pltpu.SemaphoreType.DMA((heads,)),
                pltpu.SemaphoreType.DMA((heads,)),
                pltpu.SemaphoreType.DMA,
            ],
            compiler_params=pltpu.CompilerParams(
                collective_id=0, has_side_effects=True, vmem_limit_bytes=67043328
            ),
        )(key_tiles, queries, key_rows, value_rows)

    return jax.shard_map(
        shards,
        mesh=mesh,
        in_specs=(P(("ctx", "head"), None), P(("ctx", "head"), None), P(("ctx", "head"), None), P("head", "ctx", None)),
        out_specs=P(("ctx", "head"), None),
        check_vma=False,
    )
```

```python
import functools
import math

import jax
import jax.numpy as jnp
from jax import lax
from jax.experimental import pallas as pl
from jax.experimental.pallas import tpu as pltpu
from jax.sharding import PartitionSpec as P

HDIM = 128
TILE = 128
MESH = pl.DeviceIdType.MESH
MASKED = -1e30
EXP2_SCALE = HDIM ** -0.5 / math.log(2.0)


def listed_tiles(tiles_ref, j, t, base, own):
    ids, bias = [], []
    for s in range(tiles_ref.shape[2]):
        listed = tiles_ref[j, t, s]
        live = listed >= 0
        ids.append(jnp.clip(jnp.where(live, listed - base, own + t), 0, 3 * own - 1))
        bias.append(jnp.where(live, 0.0, MASKED))
    return ids, bias


def score(qb, work, sc, ids, j, t):
    query = qb[j, t]
    top = None
    for s in range(0, len(ids), 2):
        keys = jnp.concatenate([work[0, ids[s]], work[0, ids[s + 1]]], axis=0)
        scores = lax.dot_general(query, keys, (((1,), (1,)), ((), ())), preferred_element_type=jnp.float32)
        sc[s] = scores[:, :TILE]
        sc[s + 1] = scores[:, TILE:]
        pair = jnp.maximum(scores[:, :TILE], scores[:, TILE:])
        top = pair if top is None else jnp.maximum(top, pair)
    return jnp.max(top, axis=1, keepdims=True)


def gather(work, sc, ob, ids, bias, row_max, j, t):
    total, numerator = None, None
    for s in range(0, len(ids), 2):
        first = jnp.exp2((sc[s] - row_max) * EXP2_SCALE + bias[s])
        second = jnp.exp2((sc[s + 1] - row_max) * EXP2_SCALE + bias[s + 1])
        pair = first + second
        total = pair if total is None else total + pair
        probs = jnp.concatenate([first.astype(jnp.bfloat16), second.astype(jnp.bfloat16)], axis=1)
        values = jnp.concatenate([work[1, ids[s]], work[1, ids[s + 1]]], axis=0)
        part = jnp.dot(probs, values, preferred_element_type=jnp.float32)
        numerator = part if numerator is None else numerator + part
    row_total = jnp.sum(total, axis=1, keepdims=True)
    ob[j, t] = (numerator / row_total).astype(jnp.bfloat16)


def kernel(n_ctx, n_head, listed_ref, q_ref, k_ref, v_ref, out_ref, tiles_ref, qb, kvb, passing, ob, work, sc, send_in, send_across_sem, send_halo, send_passing, send_out, recv_kv, recv_q, recv_below, recv_above, recv_passing, recv_out, recv_tiles):
    heads = tiles_ref.shape[0]
    lists = pltpu.make_async_copy(listed_ref, tiles_ref, recv_tiles)
    lists.start()
    c, me = lax.axis_index("ctx"), lax.axis_index("head")
    base = (c - 1) * n_head
    turn, last = n_ctx // 2, n_ctx - 1
    own, above, part = n_head, 2 * n_head, n_head // 2
    via = ((turn // 2 - 1, 0), (turn // 2, part))
    at_end, at_turn = (c == 0) | (c == last), (c == turn - 1) | (c == turn)
    at_via = functools.reduce(jnp.logical_or, [c == plane + place for plane in (0, turn) for place, _ in via])
    far_plane = jnp.where(c < turn, turn, 0)

    def columns(group, j):
        return pl.ds(pl.multiple_of((group * heads + j) * HDIM, HDIM), HDIM)

    def greet(ctx, head):
        pl.semaphore_signal(barrier, inc=1, device_id=(ctx, head), device_id_type=MESH)

    barrier = pltpu.get_barrier_semaphore()
    for p in range(1, n_head):
        greet(c, lax.rem(me + p, n_head))
    pl.when((c != 0) & (c != turn))(lambda: greet(c - 1, me))
    pl.when((c != last) & (c != turn - 1))(lambda: greet(c + 1, me))

    @pl.when(at_turn)
    def _():
        for group in range(n_head):
            greet(2 * turn - 1 - c, group)
        for place, _ in via:
            greet(place, me)
            greet(turn + place, me)

    @pl.when(at_via)
    def _():
        greet(turn - 1, me)
        greet(turn, me)

    greeted = jnp.where(at_end, n_head, jnp.where(at_turn, 2 * n_head + 4, jnp.where(at_via, n_head + 3, n_head + 1)))
    pl.semaphore_wait(barrier, greeted)

    def send_tile(source, place, j, sem_index, recv):
        for p in range(1, n_head):
            peer = lax.rem(me + p, n_head)
            pltpu.make_async_remote_copy(
                src_ref=source.at[:, columns(peer, j)], dst_ref=place(), send_sem=send_in.at[sem_index],
                recv_sem=recv, device_id=(c, peer), device_id_type=MESH,
            ).start()
        pltpu.make_async_copy(source.at[:, columns(me, j)], place(), recv).start()

    def send_across(j, ctx, first, recv):
        for p in range(n_head):
            group = lax.rem(me + p, n_head)
            pltpu.make_async_remote_copy(
                src_ref=k_ref.at[:, columns(group, j)], dst_ref=kvb.at[j, 0, first + me], send_sem=send_across_sem,
                recv_sem=recv.at[j], device_id=(ctx, group), device_id_type=MESH,
            ).start()

    def send_kv(j):
        send_tile(k_ref, lambda: kvb.at[j, 0, n_head + me], j, 0, recv_kv.at[j])
        send_tile(v_ref, lambda: kvb.at[j, 1, n_head + me], j, 1, recv_kv.at[j])
        pl.when(c == turn - 1)(lambda: send_across(j, turn, 0, recv_below))
        pl.when(c == turn)(lambda: send_across(j, turn - 1, above, recv_above))

    def send_q(j):
        send_tile(q_ref, lambda: qb.at[j, me], j, 2, recv_q.at[j])

    send_kv(0)
    send_kv(1)

    @pl.loop(0, heads)
    def _(j):
        @pl.when(j + 2 < heads)
        def _():
            send_kv(j + 2)

        send_q(j)

    def push(j, source, place, count, ctx, recv):
        pltpu.make_async_remote_copy(
            src_ref=kvb.at[j, :, pl.ds(source, count)], dst_ref=kvb.at[j, :, pl.ds(place, count)],
            send_sem=send_halo, recv_sem=recv.at[j], device_id=(ctx, me), device_id_type=MESH,
        ).start()

    def landed(j, first, recv):
        slab = kvb.at[j, :, pl.ds(first, n_head)]
        pltpu.make_async_copy(slab, slab, recv.at[j]).wait()

    def pass_halo(j):
        landed(j, own, recv_kv)

        @pl.when(at_turn)
        def _():
            for place, first in via:
                pltpu.make_async_remote_copy(
                    src_ref=kvb.at[j, 1, pl.ds(own + first, part)], dst_ref=passing.at[j], send_sem=send_halo,
                    recv_sem=recv_passing.at[j], device_id=(far_plane + place, me), device_id_type=MESH,
                ).start()

        pl.when((c != 0) & (c != turn))(lambda: push(j, own, above, n_head, c - 1, recv_above))
        pl.when((c != last) & (c != turn - 1))(lambda: push(j, own, 0, n_head, c + 1, recv_below))

    def relay(j):
        for plane, target, shift, recv in ((0, turn - 1, above, recv_above), (turn, turn, 0, recv_below)):
            for place, first in via:
                @pl.when(c == plane + place)
                def _():
                    pltpu.make_async_copy(passing.at[j], passing.at[j], recv_passing.at[j]).wait()
                    pltpu.make_async_remote_copy(
                        src_ref=passing.at[j], dst_ref=kvb.at[j, 1, pl.ds(shift + first, part)], send_sem=send_passing,
                        recv_sem=recv.at[j], device_id=(target, me), device_id_type=MESH,
                    ).start()

    def return_tile(j, t):
        place = out_ref.at[:, columns(me, j)]

        @pl.when(t == me)
        def _():
            pltpu.make_async_copy(ob.at[j, t], place, recv_out).start()

        @pl.when(t != me)
        def _():
            pltpu.make_async_remote_copy(
                src_ref=ob.at[j, t], dst_ref=place, send_sem=send_out,
                recv_sem=recv_out, device_id=(c, t), device_id_type=MESH,
            ).start()

    lists.wait()
    pass_halo(0)
    pass_halo(1)
    relay(0)

    @pl.loop(0, heads)
    def _(j):
        @pl.when(j + 2 < heads)
        def _():
            pass_halo(j + 2)

        pl.when(c != 0)(lambda: landed(j, 0, recv_below))
        pl.when(c != last)(lambda: landed(j, above, recv_above))
        pltpu.make_async_copy(qb.at[j], qb.at[j], recv_q.at[j]).wait()

        @pl.loop(0, 3 * n_head)
        def _(i):
            work[0, i] = kvb[j, 0, i]
            work[1, i] = kvb[j, 1, i]

        @pl.loop(0, n_head, step=2)
        def _(i):
            tiles = [lax.rem(me + 1 + i + k, n_head) for k in range(2)]
            listed = [listed_tiles(tiles_ref, j, t, base, n_head) for t in tiles]
            tops = [score(qb, work, sc.at[k], listed[k][0], j, tiles[k]) for k in range(2)]
            for k in range(2):
                gather(work, sc.at[k], ob, *listed[k], tops[k], j, tiles[k])

            @pl.when((i == 0) & (j + 1 < heads))
            def _():
                relay(j + 1)

            @pl.when(i > 0)
            def _():
                for k in range(2):
                    return_tile(j, lax.rem(me - 1 + i + k, n_head))

        return_tile(j, lax.rem(me + n_head - 1, n_head))
        return_tile(j, me)

    sent = qb.at[:, pl.ds(0, n_head - 1)]
    for i in range(3):
        pltpu.make_async_copy(sent, sent, send_in.at[i]).wait()
    halo, half = kvb.at[:, :, pl.ds(0, n_head)], kvb.at[:, 0, pl.ds(0, n_head)]
    pltpu.make_async_copy(halo, halo, send_halo).wait()
    pl.when(~(at_end | at_turn))(lambda: pltpu.make_async_copy(halo, halo, send_halo).wait())

    @pl.when(at_turn)
    def _():
        pltpu.make_async_copy(half, half, send_halo).wait()
        pltpu.make_async_copy(qb, qb, send_across_sem).wait()

    pl.when(at_via)(lambda: pltpu.make_async_copy(passing, passing, send_passing).wait())
    pltpu.make_async_copy(sent, sent, send_out).wait()
    pltpu.make_async_copy(out_ref, out_ref, recv_out).wait()


def solution(mesh):
    n_ctx, n_head = mesh.shape["ctx"], mesh.shape["head"]

    def shards(queries, key_rows, value_rows, key_tiles):
        heads, _, slots = key_tiles.shape
        return pl.pallas_call(
            functools.partial(kernel, n_ctx, n_head),
            out_shape=jax.ShapeDtypeStruct(queries.shape, queries.dtype),
            in_specs=[pl.BlockSpec(memory_space=pltpu.HBM)] * 4,
            out_specs=pl.BlockSpec(memory_space=pltpu.HBM),
            scratch_shapes=[
                pltpu.SMEM(key_tiles.shape, jnp.int32),
                pltpu.VMEM((heads, n_head, TILE, HDIM), jnp.bfloat16),
                pltpu.VMEM((heads, 2, 3 * n_head, TILE, HDIM), jnp.bfloat16),
                pltpu.VMEM((heads, n_head // 2, TILE, HDIM), jnp.bfloat16),
                pltpu.VMEM((heads, n_head, TILE, HDIM), jnp.bfloat16),
                pltpu.VMEM((2, 3 * n_head, TILE, HDIM), jnp.bfloat16),
                pltpu.VMEM((2, slots, TILE, TILE), jnp.float32),
                pltpu.SemaphoreType.DMA((3,)),
                pltpu.SemaphoreType.DMA,
                pltpu.SemaphoreType.DMA,
                pltpu.SemaphoreType.DMA,
                pltpu.SemaphoreType.DMA,
                pltpu.SemaphoreType.DMA((heads,)),
                pltpu.SemaphoreType.DMA((heads,)),
                pltpu.SemaphoreType.DMA((heads,)),
                pltpu.SemaphoreType.DMA((heads,)),
                pltpu.SemaphoreType.DMA((heads,)),
                pltpu.SemaphoreType.DMA,
                pltpu.SemaphoreType.DMA,
            ],
            compiler_params=pltpu.CompilerParams(
                collective_id=0, has_side_effects=True, vmem_limit_bytes=67043328
            ),
        )(key_tiles, queries, key_rows, value_rows)

    return jax.shard_map(
        shards,
        mesh=mesh,
        in_specs=(P(("ctx", "head"), None), P(("ctx", "head"), None), P(("ctx", "head"), None), P("head", "ctx", None)),
        out_specs=P(("ctx", "head"), None),
        check_vma=False,
    )
```

```python
import functools
import math

import jax
import jax.numpy as jnp
from jax import lax
from jax.experimental import pallas as pl
from jax.experimental.pallas import tpu as pltpu
from jax.sharding import PartitionSpec as P

HDIM = 128
TILE = 128
MESH = pl.DeviceIdType.MESH
MASKED = -1e30
EXP2_SCALE = HDIM ** -0.5 / math.log(2.0)


def listed_tiles(tiles_ref, j, t, base, own):
    ids, bias = [], []
    for s in range(tiles_ref.shape[2]):
        listed = tiles_ref[j, t, s]
        live = listed >= 0
        ids.append(jnp.clip(jnp.where(live, listed - base, own + t), 0, 3 * own - 1))
        bias.append(jnp.where(live, 0.0, MASKED))
    return ids, bias


def score(qb, work, sc, ids, bias, j, t):
    query = qb[j, t]
    top = None
    for s in range(0, len(ids), 2):
        keys = jnp.concatenate([work[0, ids[s]], work[0, ids[s + 1]]], axis=0)
        scores = lax.dot_general(query, keys, (((1,), (1,)), ((), ())), preferred_element_type=jnp.float32)
        scores = scores * EXP2_SCALE
        first, second = scores[:, :TILE] + bias[s], scores[:, TILE:] + bias[s + 1]
        sc[s] = first
        sc[s + 1] = second
        pair = jnp.maximum(first, second)
        top = pair if top is None else jnp.maximum(top, pair)
    return jnp.max(top, axis=1, keepdims=True)


def gather(work, sc, ob, ids, row_max, j, t):
    total, numerator = None, None
    for s in range(0, len(ids), 2):
        first = jnp.exp2(sc[s] - row_max)
        second = jnp.exp2(sc[s + 1] - row_max)
        pair = first + second
        total = pair if total is None else total + pair
        probs = jnp.concatenate([first.astype(jnp.bfloat16), second.astype(jnp.bfloat16)], axis=1)
        values = jnp.concatenate([work[1, ids[s]], work[1, ids[s + 1]]], axis=0)
        part = jnp.dot(probs, values, preferred_element_type=jnp.float32)
        numerator = part if numerator is None else numerator + part
    row_total = jnp.sum(total, axis=1, keepdims=True)
    ob[j, t] = (numerator / row_total).astype(jnp.bfloat16)


def kernel(n_ctx, n_head, listed_ref, q_ref, k_ref, v_ref, out_ref, tiles_ref, qb, kvb, passing, ob, work, sc, send_in, send_across_sem, send_halo, send_passing, send_out, recv_kv, recv_q, recv_below, recv_above, recv_passing, recv_out, recv_tiles):
    heads = tiles_ref.shape[0]
    lists = pltpu.make_async_copy(listed_ref, tiles_ref, recv_tiles)
    lists.start()
    c, me = lax.axis_index("ctx"), lax.axis_index("head")
    base = (c - 1) * n_head
    turn, last = n_ctx // 2, n_ctx - 1
    own, above, part = n_head, 2 * n_head, n_head // 2
    via = ((turn // 2 - 1, 0), (turn // 2, part))
    at_end, at_turn = (c == 0) | (c == last), (c == turn - 1) | (c == turn)
    at_via = functools.reduce(jnp.logical_or, [c == plane + place for plane in (0, turn) for place, _ in via])
    far_plane = jnp.where(c < turn, turn, 0)

    def columns(group, j):
        return pl.ds(pl.multiple_of((group * heads + j) * HDIM, HDIM), HDIM)

    def greet(ctx, head):
        pl.semaphore_signal(barrier, inc=1, device_id=(ctx, head), device_id_type=MESH)

    barrier = pltpu.get_barrier_semaphore()
    for p in range(1, n_head):
        greet(c, lax.rem(me + p, n_head))
    pl.when((c != 0) & (c != turn))(lambda: greet(c - 1, me))
    pl.when((c != last) & (c != turn - 1))(lambda: greet(c + 1, me))

    @pl.when(at_turn)
    def _():
        for group in range(n_head):
            greet(2 * turn - 1 - c, group)
        for place, _ in via:
            greet(place, me)
            greet(turn + place, me)

    @pl.when(at_via)
    def _():
        greet(turn - 1, me)
        greet(turn, me)

    greeted = jnp.where(at_end, n_head, jnp.where(at_turn, 2 * n_head + 4, jnp.where(at_via, n_head + 3, n_head + 1)))
    pl.semaphore_wait(barrier, greeted)

    def send_tile(source, place, j, sem_index, recv):
        for p in (4, 3, 5, 2, 6, 1, 7):
            peer = lax.rem(me + p, n_head)
            pltpu.make_async_remote_copy(
                src_ref=source.at[:, columns(peer, j)], dst_ref=place(), send_sem=send_in.at[sem_index],
                recv_sem=recv, device_id=(c, peer), device_id_type=MESH,
            ).start()
        pltpu.make_async_copy(source.at[:, columns(me, j)], place(), recv).start()

    def send_across(j, ctx, first, recv):
        for p in range(n_head):
            group = lax.rem(me + p, n_head)
            pltpu.make_async_remote_copy(
                src_ref=k_ref.at[:, columns(group, j)], dst_ref=kvb.at[j, 0, first + me], send_sem=send_across_sem,
                recv_sem=recv.at[j], device_id=(ctx, group), device_id_type=MESH,
            ).start()

    def send_kv(j):
        pl.when(c == turn - 1)(lambda: send_across(j, turn, 0, recv_below))
        pl.when(c == turn)(lambda: send_across(j, turn - 1, above, recv_above))
        send_tile(k_ref, lambda: kvb.at[j, 0, n_head + me], j, 0, recv_kv.at[j])
        send_tile(v_ref, lambda: kvb.at[j, 1, n_head + me], j, 1, recv_kv.at[j])

    def send_q(j):
        send_tile(q_ref, lambda: qb.at[j, me], j, 2, recv_q.at[j])

    send_kv(0)
    send_kv(1)

    @pl.loop(0, heads)
    def _(j):
        @pl.when(j + 2 < heads)
        def _():
            send_kv(j + 2)

        send_q(j)

    def push(j, source, place, count, ctx, recv):
        pltpu.make_async_remote_copy(
            src_ref=kvb.at[j, :, pl.ds(source, count)], dst_ref=kvb.at[j, :, pl.ds(place, count)],
            send_sem=send_halo, recv_sem=recv.at[j], device_id=(ctx, me), device_id_type=MESH,
        ).start()

    def landed(j, first, recv):
        slab = kvb.at[j, :, pl.ds(first, n_head)]
        pltpu.make_async_copy(slab, slab, recv.at[j]).wait()

    def pass_halo(j):
        landed(j, own, recv_kv)

        @pl.when(at_turn)
        def _():
            for place, first in via:
                pltpu.make_async_remote_copy(
                    src_ref=kvb.at[j, 1, pl.ds(own + first, part)], dst_ref=passing.at[j], send_sem=send_halo,
                    recv_sem=recv_passing.at[j], device_id=(far_plane + place, me), device_id_type=MESH,
                ).start()

        pl.when((c != 0) & (c != turn))(lambda: push(j, own, above, n_head, c - 1, recv_above))
        pl.when((c != last) & (c != turn - 1))(lambda: push(j, own, 0, n_head, c + 1, recv_below))

    def relay(j):
        for plane, target, shift, recv in ((0, turn - 1, above, recv_above), (turn, turn, 0, recv_below)):
            for place, first in via:
                @pl.when(c == plane + place)
                def _():
                    pltpu.make_async_copy(passing.at[j], passing.at[j], recv_passing.at[j]).wait()
                    pltpu.make_async_remote_copy(
                        src_ref=passing.at[j], dst_ref=kvb.at[j, 1, pl.ds(shift + first, part)], send_sem=send_passing,
                        recv_sem=recv.at[j], device_id=(target, me), device_id_type=MESH,
                    ).start()

    def return_tile(j, t):
        place = out_ref.at[:, columns(me, j)]

        @pl.when(t == me)
        def _():
            pltpu.make_async_copy(ob.at[j, t], place, recv_out).start()

        @pl.when(t != me)
        def _():
            pltpu.make_async_remote_copy(
                src_ref=ob.at[j, t], dst_ref=place, send_sem=send_out,
                recv_sem=recv_out, device_id=(c, t), device_id_type=MESH,
            ).start()

    lists.wait()
    pass_halo(0)
    pass_halo(1)
    relay(0)

    @pl.loop(0, heads)
    def _(j):
        @pl.when(j + 2 < heads)
        def _():
            pass_halo(j + 2)

        pl.when(c != 0)(lambda: landed(j, 0, recv_below))
        pl.when(c != last)(lambda: landed(j, above, recv_above))
        pltpu.make_async_copy(qb.at[j], qb.at[j], recv_q.at[j]).wait()

        @pl.loop(0, 3 * n_head)
        def _(i):
            work[0, i] = kvb[j, 0, i]
            work[1, i] = kvb[j, 1, i]

        @pl.loop(0, n_head, step=2)
        def _(i):
            tiles = [lax.rem(me + 1 + i + k, n_head) for k in range(2)]
            listed = [listed_tiles(tiles_ref, j, t, base, n_head) for t in tiles]
            tops = [score(qb, work, sc.at[k], *listed[k], j, tiles[k]) for k in range(2)]
            for k in range(2):
                gather(work, sc.at[k], ob, listed[k][0], tops[k], j, tiles[k])

            @pl.when((i == 0) & (j + 1 < heads))
            def _():
                relay(j + 1)

            @pl.when(i > 0)
            def _():
                for k in range(2):
                    return_tile(j, lax.rem(me - 1 + i + k, n_head))

        return_tile(j, lax.rem(me + n_head - 1, n_head))
        return_tile(j, me)

    sent = qb.at[:, pl.ds(0, n_head - 1)]
    for i in range(3):
        pltpu.make_async_copy(sent, sent, send_in.at[i]).wait()
    halo, half = kvb.at[:, :, pl.ds(0, n_head)], kvb.at[:, 0, pl.ds(0, n_head)]
    pltpu.make_async_copy(halo, halo, send_halo).wait()
    pl.when(~(at_end | at_turn))(lambda: pltpu.make_async_copy(halo, halo, send_halo).wait())

    @pl.when(at_turn)
    def _():
        pltpu.make_async_copy(half, half, send_halo).wait()
        pltpu.make_async_copy(qb, qb, send_across_sem).wait()

    pl.when(at_via)(lambda: pltpu.make_async_copy(passing, passing, send_passing).wait())
    pltpu.make_async_copy(sent, sent, send_out).wait()
    pltpu.make_async_copy(out_ref, out_ref, recv_out).wait()


def solution(mesh):
    n_ctx, n_head = mesh.shape["ctx"], mesh.shape["head"]

    def shards(queries, key_rows, value_rows, key_tiles):
        heads, _, slots = key_tiles.shape
        return pl.pallas_call(
            functools.partial(kernel, n_ctx, n_head),
            out_shape=jax.ShapeDtypeStruct(queries.shape, queries.dtype),
            in_specs=[pl.BlockSpec(memory_space=pltpu.HBM)] * 4,
            out_specs=pl.BlockSpec(memory_space=pltpu.HBM),
            scratch_shapes=[
                pltpu.SMEM(key_tiles.shape, jnp.int32),
                pltpu.VMEM((heads, n_head, TILE, HDIM), jnp.bfloat16),
                pltpu.VMEM((heads, 2, 3 * n_head, TILE, HDIM), jnp.bfloat16),
                pltpu.VMEM((heads, n_head // 2, TILE, HDIM), jnp.bfloat16),
                pltpu.VMEM((heads, n_head, TILE, HDIM), jnp.bfloat16),
                pltpu.VMEM((2, 3 * n_head, TILE, HDIM), jnp.bfloat16),
                pltpu.VMEM((2, slots, TILE, TILE), jnp.float32),
                pltpu.SemaphoreType.DMA((3,)),
                pltpu.SemaphoreType.DMA,
                pltpu.SemaphoreType.DMA,
                pltpu.SemaphoreType.DMA,
                pltpu.SemaphoreType.DMA,
                pltpu.SemaphoreType.DMA((heads,)),
                pltpu.SemaphoreType.DMA((heads,)),
                pltpu.SemaphoreType.DMA((heads,)),
                pltpu.SemaphoreType.DMA((heads,)),
                pltpu.SemaphoreType.DMA((heads,)),
                pltpu.SemaphoreType.DMA,
                pltpu.SemaphoreType.DMA,
            ],
            compiler_params=pltpu.CompilerParams(
                collective_id=0, has_side_effects=True, vmem_limit_bytes=67043328
            ),
        )(key_tiles, queries, key_rows, value_rows)

    return jax.shard_map(
        shards,
        mesh=mesh,
        in_specs=(P(("ctx", "head"), None), P(("ctx", "head"), None), P(("ctx", "head"), None), P("head", "ctx", None)),
        out_specs=P(("ctx", "head"), None),
        check_vma=False,
    )
```
